32 devices in a mesh: pair: 4 (over z), aux: 8 (over y, x, core).
Axes of the slice: x: 2, y: 2, z: 4, core: 2. Of those that a mesh axis runs over, the one named last changes fastest.
Arguments:
- integrals: bfloat16 [12288, 12288], P('pair', 'aux'), may hold values from -0.1875 to 0.1875
- energy_gaps: float32 [12288], P('pair'), may hold values from 0.3 to 3
- trial_vectors: float32 [12288, 64], P('pair'), may hold values from -160 to 160
Outputs:
- sigma_vectors: float32 [12288, 64], P(('pair', 'aux'))
- subspace: float32 [64, 64], replicated
- residuals: float32 [12288, 64], P(('pair', 'aux'))
- residual_norms: float32 [64], replicated
The draws below stay inside these ranges and needn't reach their ends.
All inputs are finite; a program needn't handle non-finite values.
Results may differ from the reference program's by a relative error of at most 0.0052.
Values may be sent and summed in bfloat16 or wider, within the bound.
A program may use at most 64 MiB of HBM per device.

```python
import math
import jax
import jax.numpy as jnp
from jax import lax

NAUX = 12288
NVEC = 64
PAIRS = 12288


def draw_trial_vectors(key, part):
    key_entries = jax.random.fold_in(key, 11)
    key_rows = jax.random.fold_in(key, 12)
    key_columns = jax.random.fold_in(key, 13)
    positions = jnp.arange(PAIRS).astype(jnp.float32)
    growth = jnp.exp(jnp.log(3.0) * positions / PAIRS)
    row_scale = jnp.exp(jax.random.uniform(key_rows, (PAIRS,), jnp.float32, jnp.log(0.3), jnp.log(3.0)))
    entries = jnp.clip(jax.random.normal(key_entries, (PAIRS, NVEC), jnp.float32), -5.0, 5.0)
    column_scale = jnp.exp(jax.random.uniform(key_columns, (NVEC,), jnp.float32, jnp.log(0.3), jnp.log(3.0)))
    return (entries * (growth * row_scale)[:, None] * column_scale[None, :]).astype(jnp.float32)


def spiked(values, rng, source, target, blocks, factor):
    def block_of(dim):
        return (jnp.arange(values.shape[dim]) // (values.shape[dim] // blocks)).reshape((-1,) + (1,) * (values.ndim - 1 - dim))

    first = jax.random.permutation(rng, blocks)[block_of(target)]
    second = (block_of(target) + blocks // 2) % blocks
    return jnp.where((block_of(source) == first) | (block_of(source) == second), factor * values, values)


def block_levels(rng, extent, split, low, high):
    factor_of, own = 1.0, jax.random.fold_in(rng, 6)
    for dim, blocks in split:
        heights = jnp.exp(jax.random.uniform(jax.random.fold_in(own, dim), (blocks,), jnp.float32, low / len(split), high / len(split)))
        factor_of = factor_of * jnp.repeat(heights, extent[dim] // blocks).reshape([-1 if axis == dim else 1 for axis in range(len(extent))])
    return factor_of


def heavy_noise(rng, shape, spread, limit, pieces, heavy, held_as=jnp.bfloat16):
    values = spread * jax.random.normal(rng, shape, jnp.float32)
    if pieces:
        values = values * block_levels(rng, shape, pieces, -0.22, 0.18)
    return jnp.clip(spiked(values, jax.random.fold_in(rng, 3), *heavy), -limit, limit).astype(held_as)


def setup_inputs(seed: int = 0) -> dict:
    streams_of = jax.random.split(jax.random.key(seed), 4)
    return {
        "integrals": heavy_noise(streams_of[0], (PAIRS, NAUX), (1.0 / (PAIRS * NAUX) ** 0.25), 0.1875, ((0, 4), (1, 8)), (0, 1, 8, 2.0)),
        "energy_gaps": jnp.clip(jnp.exp(math.log(3.0) - 2.3025851 * jax.random.uniform(streams_of[1], (PAIRS,), jnp.float32) ** block_levels(streams_of[1], (PAIRS,), ((0, 4),), -0.2, 0.2)), 0.3, 3.0),
        "trial_vectors": draw_trial_vectors(jax.random.fold_in(streams_of[3], 71), 0),
    }


epsilon = 1e-06

def reference(integrals, energy_gaps, trial_vectors):
    trial_half = trial_vectors.astype(jnp.bfloat16)
    aux_totals = lax.dot_general(integrals, trial_half, (((0,), (0,)), ((), ())), preferred_element_type=jnp.float32)
    aux_half = aux_totals.astype(jnp.bfloat16)
    coupled = jnp.dot(integrals, aux_half, preferred_element_type=jnp.float32)
    sigma_vectors = energy_gaps[:, None] * trial_vectors + 2.0 * coupled
    subspace = lax.dot_general(trial_vectors, sigma_vectors, (((0,), (0,)), ((), ())), precision=lax.Precision.HIGHEST, preferred_element_type=jnp.float32) / PAIRS
    intersection = lax.optimization_barrier(jnp.sum(trial_vectors * trial_vectors, axis=0)) / PAIRS
    rayleigh = jnp.diagonal(subspace) / (intersection + epsilon)
    residuals = sigma_vectors - trial_vectors * rayleigh[None, :]
    residual_norms = jnp.sqrt(lax.optimization_barrier(jnp.sum(residuals * residuals, axis=0)) / PAIRS + epsilon)
    return (sigma_vectors, subspace, residuals, residual_norms)
```

```python
import functools

import jax
import jax.numpy as jnp
from jax import lax
from jax.experimental import pallas as pl
from jax.experimental.pallas import tpu as pltpu
from jax.sharding import PartitionSpec as P

epsilon = 1e-06
MESH = pl.DeviceIdType.MESH
f32, bf16 = jnp.float32, jnp.bfloat16
LAG = 2
NT = (((1,), (1,)), ((), ()))


def exact(a, b):
    return lax.dot_general(a, b, NT, precision=lax.Precision.HIGHEST, preferred_element_type=f32)


def kernel(
    np_, na, chunks, width, share,
    ints_hbm, gaps_hbm, trial_hbm,
    sigma_hbm, sub_hbm, res_hbm, norm_hbm,
    ints, gaps, trial, half, own, acc, mat, gram,
    pre_in, pre_out, suf_in, suf_out,
    b1_out, b1_in, b2_out, b2_in,
    m1_out, m1_in, m2, m3, n1, n2,
    sigma, sub, res, norm,
    load, aload, pre_s, pre_r, suf_s, suf_r,
    b1_s, b1_r, b2_s, b2_r, m1_s, m1_r, m2_s, m2_r, m3_s, m3_r, n1_s, n1_r, n2_s, n2_r, store,
):
    z, a = lax.axis_index("pair"), lax.axis_index("aux")
    core, chip, chips = a % 2, a // 2, na // 2
    vecs = trial.shape[0]

    trial_load = pltpu.make_async_copy(trial_hbm, trial, aload.at[0])
    gaps_load = pltpu.make_async_copy(gaps_hbm, gaps, aload.at[1])
    trial_load.start()
    loads = [
        pltpu.make_async_copy(ints_hbm.at[:, pl.ds(c * width, width)], ints.at[c], load.at[c])
        for c in range(chunks)
    ]
    loads[0].start()
    gaps_load.start()
    for c in range(1, chunks):
        loads[c].start()

    barrier = pltpu.get_barrier_semaphore()
    for d in range(1, np_):
        pl.semaphore_signal(barrier, inc=1, device_id={"pair": (z + d) % np_, "aux": a}, device_id_type=MESH)
    for d in range(1, na):
        pl.semaphore_signal(barrier, inc=1, device_id={"pair": z, "aux": (a + d) % na}, device_id_type=MESH)

    def remote(src, dst, s, r, pair, aux):
        return pltpu.make_async_remote_copy(
            src_ref=src, dst_ref=dst, send_sem=s, recv_sem=r,
            device_id={"pair": pair, "aux": aux}, device_id_type=MESH,
        )

    def prefix(c):
        return remote(pre_out.at[c], pre_in.at[c], pre_s.at[c], pre_r.at[c], z + 1, a)

    def suffix(c):
        return remote(suf_out.at[c], suf_in.at[c], suf_s.at[c], suf_r.at[c], z - 1, a)

    acc[...] = jnp.zeros_like(acc)
    mat[...] = jnp.zeros_like(mat)
    trial_load.wait()
    half[...] = trial[...].astype(bf16)
    gaps_load.wait()
    first = pl.multiple_of(a * share, 128)
    rows = share // 128

    def own_trial():
        return trial[:, pl.ds(first, share)]

    def own_gaps():
        return jnp.concatenate([gaps[pl.ds(a * rows + q, 1), :] for q in range(rows)], axis=1)

    eye = lax.broadcasted_iota(jnp.int32, (vecs, vecs), 0) == lax.broadcasted_iota(jnp.int32, (vecs, vecs), 1)

    def as_row(column):
        return jnp.sum(jnp.where(eye, column, 0.0), axis=0, keepdims=True)

    mine = own_trial()
    gram[...] = exact(mine, mine * own_gaps())
    pl.semaphore_wait(barrier, np_ - 1 + na - 1)

    after = np_ - 1 - z
    longest = jnp.maximum(z, after)

    def step(t, carry):
        @pl.when(t < chunks)
        def _():
            pltpu.make_async_copy(ints_hbm.at[:, pl.ds(0, width)], ints.at[t], load.at[t]).wait()
            own[t] = jnp.dot(half[...], ints[t], preferred_element_type=f32)

        p = t - LAG * z

        @pl.when((p >= 0) & (p < chunks) & (after > 0))
        def _():
            @pl.when(z == 0)
            def _():
                pre_out[p] = own[p].astype(bf16)

            @pl.when(z > 0)
            def _():
                prefix(p).wait_recv()
                pre_out[p] = (own[p] + pre_in[p].astype(f32)).astype(bf16)

            prefix(p).start()

        s = t - LAG * after

        @pl.when((s >= 0) & (s < chunks) & (z > 0))
        def _():
            @pl.when(after == 0)
            def _():
                suf_out[s] = own[s].astype(bf16)

            @pl.when(after > 0)
            def _():
                suffix(s).wait_recv()
                suf_out[s] = (own[s] + suf_in[s].astype(f32)).astype(bf16)

            suffix(s).start()

        c = t - LAG * longest

        @pl.when((c >= 0) & (c < chunks))
        def _():
            @pl.when(z == np_ - 1)
            def _():
                prefix(c).wait_recv()

            @pl.when(z == 0)
            def _():
                suffix(c).wait_recv()

            @pl.when(z > 0)
            def _():
                own[c] = own[c] + pre_in[c].astype(f32)

            @pl.when(after > 0)
            def _():
                own[c] = own[c] + suf_in[c].astype(f32)

            aux = own[c].astype(bf16)
            for b in range(chips):
                part = lax.dot_general(
                    aux, ints[c, pl.ds(b * 2 * share, 2 * share), :], NT, preferred_element_type=f32
                )
                acc[2 * b] += part[:, :share]
                acc[2 * b + 1] += part[:, share:]

            @pl.when(c % np_ == z)
            def _():
                total = own[c]
                mat[...] += exact(total, total.astype(bf16).astype(f32))

        return carry

    lax.fori_loop(0, chunks + LAG * (np_ - 1), step, 0)

    other = chip * 2 + 1 - core
    pending = []
    product = gram[...] + 2.0 * mat[...]
    mine = own_trial()
    squares = as_row(jnp.sum(mine * mine, axis=1, keepdims=True))
    h = vecs // 2
    m1_out[0:h] = jnp.concatenate([product[:h], product[h:]], axis=1)
    m1_out[h:] = jnp.broadcast_to(jnp.concatenate([squares, squares], axis=1), (8, 2 * vecs))
    m1_copy = remote(m1_out, m1_in, m1_s, m1_r, z, other)
    m1_copy.start()
    pending.append(m1_copy)

    b1 = []
    for d in range(chips):
        j = (chip + 1 + d) % chips
        b1_out[d] = acc[2 * j + 1 - core].astype(bf16)
        copy = remote(b1_out.at[d], b1_in.at[d], b1_s.at[d], b1_r.at[d], z, other)
        copy.start()
        b1.append(copy)
        pending.append(copy)
    m1_copy.wait_recv()
    m2[chip] = m1_out[...] + m1_in[...]
    for d in range(1, chips):
        copy = remote(m2.at[chip], m2.at[chip], m2_s.at[d], m2_r.at[chip], z, ((chip + d) % chips) * 2 + core)
        copy.start()
        pending.append(copy)
    for d in range(chips - 1):
        j = (chip + 1 + d) % chips
        b1[d].wait_recv()
        b2_out[d] = (acc[2 * j + core] + b1_in[d].astype(f32)).astype(bf16)
        copy = remote(b2_out.at[d], b2_in.at[d], b2_s.at[d], b2_r.at[d], z, 2 * j + core)
        copy.start()
        pending.append(copy)
    b1[chips - 1].wait_recv()
    coupled = acc[a] + b1_in[chips - 1].astype(f32)

    for d in range(1, chips):
        j = (chip + d) % chips
        remote(m2.at[j], m2.at[j], m2_s.at[d], m2_r.at[j], z, a).wait_recv()
    total = m2[0]
    for j in range(1, chips):
        total = total + m2[j]
    m3[z] = total
    for d in range(1, np_):
        copy = remote(m3.at[z], m3.at[z], m3_s.at[d], m3_r.at[z], (z + d) % np_, a)
        copy.start()
        pending.append(copy)

    for d in range(chips - 1):
        remote(b2_out.at[d], b2_in.at[d], b2_s.at[d], b2_r.at[d], z, a).wait_recv()
        coupled = coupled + b2_in[d].astype(f32)
    mine = own_trial()
    values = own_gaps() * mine + 2.0 * coupled
    sigma[...] = values
    lane = lax.broadcasted_iota(jnp.int32, (vecs, 128), 1)
    sums = jnp.where(
        lane == 0,
        jnp.sum(values * values, axis=1, keepdims=True),
        jnp.where(lane == 1, jnp.sum(values * mine, axis=1, keepdims=True), 0.0),
    )
    n1[a] = jnp.transpose(sums)[:8]
    for d in range(1, na):
        copy = remote(n1.at[a], n1.at[a], n1_s.at[d], n1_r.at[a], z, (a + d) % na)
        copy.start()
        pending.append(copy)
    outs = [pltpu.make_async_copy(sigma, sigma_hbm, store.at[0])]
    outs[0].start()
    for d in range(1, na):
        j = (a + d) % na
        remote(n1.at[j], n1.at[j], n1_s.at[d], n1_r.at[j], z, j).wait_recv()
    sums = n1[0]
    for j in range(1, na):
        sums = sums + n1[j]
    n2[z] = sums
    for d in range(1, np_):
        copy = remote(n2.at[z], n2.at[z], n2_s.at[d], n2_r.at[z], (z + d) % np_, a)
        copy.start()
        pending.append(copy)

    for d in range(1, np_):
        j = (z + d) % np_
        remote(m3.at[j], m3.at[j], m3_s.at[d], m3_r.at[j], j, a).wait_recv()
    total = m3[0]
    for j in range(1, np_):
        total = total + m3[j]
    pairs = float(np_ * na * share)
    subspace = jnp.concatenate([total[:h, :vecs], total[:h, vecs:]], axis=0) / pairs
    sub[...] = subspace
    outs.append(pltpu.make_async_copy(sub, sub_hbm, store.at[1]))
    outs[1].start()
    squares = total[h:h + 1, :vecs]
    diagonal = jnp.sum(jnp.where(eye, subspace, 0.0), axis=0, keepdims=True)
    rayleigh = diagonal / (squares / pairs + epsilon)
    column = jnp.sum(jnp.where(eye, rayleigh, 0.0), axis=1, keepdims=True)
    res[...] = sigma[...] - own_trial() * column
    outs.append(pltpu.make_async_copy(res, res_hbm, store.at[2]))
    outs[2].start()

    for d in range(1, np_):
        j = (z + d) % np_
        remote(n2.at[j], n2.at[j], n2_s.at[d], n2_r.at[j], j, a).wait_recv()
    sums = n2[0]
    for j in range(1, np_):
        sums = sums + n2[j]
    residual_sq = sums[0:1] - 2.0 * rayleigh * sums[1:2] + rayleigh * rayleigh * squares
    norm[...] = jnp.sqrt(residual_sq / pairs + epsilon)
    outs.append(pltpu.make_async_copy(norm, norm_hbm, store.at[3]))
    outs[3].start()

    @pl.when(after > 0)
    def _():
        for c in range(chunks):
            prefix(c).wait_send()

    @pl.when(z > 0)
    def _():
        for c in range(chunks):
            suffix(c).wait_send()

    for copy in pending:
        copy.wait_send()
    for copy in outs:
        copy.wait()


def solution(mesh):
    np_, na = mesh.shape["pair"], mesh.shape["aux"]
    chips = na // 2

    def local(integrals, energy_gaps, trial_vectors):
        rows, cols = integrals.shape
        vecs = trial_vectors.shape[1]
        width = 256
        chunks, share = cols // width, rows // na
        anywhere = pl.BlockSpec(memory_space=pl.ANY)
        dma = pltpu.SemaphoreType.DMA
        message = (vecs // 2 + 8, 2 * vecs)
        sigma, subspace, residuals, norms = pl.pallas_call(
            functools.partial(kernel, np_, na, chunks, width, share),
            out_shape=[
                jax.ShapeDtypeStruct((vecs, share), f32),
                jax.ShapeDtypeStruct((vecs, vecs), f32),
                jax.ShapeDtypeStruct((vecs, share), f32),
                jax.ShapeDtypeStruct((1, vecs), f32),
            ],
            in_specs=[pl.BlockSpec(memory_space=pltpu.HBM)] * 3,
            out_specs=[anywhere] * 4,
            scratch_shapes=[
                pltpu.VMEM((chunks, rows, width), bf16),
                pltpu.VMEM((rows // 128, 128), f32),
                pltpu.VMEM((vecs, rows), f32),
                pltpu.VMEM((vecs, rows), bf16),
                pltpu.VMEM((chunks, vecs, width), f32),
                pltpu.VMEM((na, vecs, share), f32),
                pltpu.VMEM((vecs, vecs), f32),
                pltpu.VMEM((vecs, vecs), f32),
                *[pltpu.VMEM((chunks, vecs, width), bf16)] * 4,
                *[pltpu.VMEM((chips, vecs, share), bf16)] * 4,
                pltpu.VMEM(message, f32),
                pltpu.VMEM(message, f32),
                pltpu.VMEM((chips,) + message, f32),
                pltpu.VMEM((np_,) + message, f32),
                pltpu.VMEM((na, 8, vecs), f32),
                pltpu.VMEM((np_, 8, vecs), f32),
                pltpu.VMEM((vecs, share), f32),
                pltpu.VMEM((vecs, vecs), f32),
                pltpu.VMEM((vecs, share), f32),
                pltpu.VMEM((1, vecs), f32),
                dma((chunks,)), dma((2,)),
                dma((chunks,)), dma((chunks,)), dma((chunks,)), dma((chunks,)),
                dma((chips,)), dma((chips,)), dma((chips,)), dma((chips,)),
                dma, dma, dma((chips,)), dma((chips,)),
                dma((np_,)), dma((np_,)), dma((na,)), dma((na,)), dma((np_,)), dma((np_,)),
                dma((4,)),
            ],
            compiler_params=pltpu.CompilerParams(
                collective_id=0, has_side_effects=True, vmem_limit_bytes=40 * 1024 * 1024
            ),
            name="sigma_build",
        )(integrals, energy_gaps.reshape(rows // 128, 128), trial_vectors.T)
        return sigma.T, subspace, residuals.T, norms.reshape(vecs)

    return jax.shard_map(
        local,
        mesh=mesh,
        in_specs=(P("pair", "aux"), P("pair"), P("pair", None)),
        out_specs=(P(("pair", "aux"), None), P(), P(("pair", "aux"), None), P()),
        check_vma=False,
    )
```

```python
import functools

import jax
import jax.numpy as jnp
from jax import lax
from jax.experimental import pallas as pl
from jax.experimental.pallas import tpu as pltpu
from jax.sharding import PartitionSpec as P

epsilon = 1e-06
MESH = pl.DeviceIdType.MESH
f32, bf16 = jnp.float32, jnp.bfloat16
WIDTH = 256
VMEM = 67043328
LAG = 3
NT = (((1,), (1,)), ((), ()))


def exact(a, b):
    return lax.dot_general(a, b, NT, precision=lax.Precision.HIGHEST, preferred_element_type=f32)


def kernel(
    np_, na, chunks, width, share,
    ints_hbm, gaps_hbm, trial_hbm,
    sigma_hbm, sub_hbm, res_hbm, norm_hbm,
    ints, gaps, trial, half, own, acc, mat, gram,
    pre_in, pre_out, suf_in, suf_out,
    b1_out, b1_in, b2_out, b2_in,
    m1_out, m1_in, m2, m3, n1, n2,
    sigma, sub, res, norm,
    load, aload, pre_s, pre_r, suf_s, suf_r,
    b1_s, b1_r, b2_s, b2_r, m1_s, m1_r, m2_s, m2_r, m3_s, m3_r, n1_s, n1_r, n2_s, n2_r, store,
):
    z, a = lax.axis_index("pair"), lax.axis_index("aux")
    core, chip, chips = a % 2, a // 2, na // 2
    vecs = trial.shape[0]

    trial_load = pltpu.make_async_copy(trial_hbm, trial, aload.at[0])
    gaps_load = pltpu.make_async_copy(gaps_hbm, gaps, aload.at[1])
    trial_load.start()
    loads = [
        pltpu.make_async_copy(ints_hbm.at[:, pl.ds(c * width, width)], ints.at[c], load.at[c])
        for c in range(chunks)
    ]
    loads[0].start()
    gaps_load.start()
    for c in range(1, chunks):
        loads[c].start()

    barrier = pltpu.get_barrier_semaphore()
    for d in range(1, np_):
        pl.semaphore_signal(barrier, inc=1, device_id={"pair": (z + d) % np_, "aux": a}, device_id_type=MESH)
    for d in range(1, na):
        pl.semaphore_signal(barrier, inc=1, device_id={"pair": z, "aux": (a + d) % na}, device_id_type=MESH)

    def remote(src, dst, s, r, pair, aux):
        return pltpu.make_async_remote_copy(
            src_ref=src, dst_ref=dst, send_sem=s, recv_sem=r,
            device_id={"pair": pair, "aux": aux}, device_id_type=MESH,
        )

    def prefix(c):
        return remote(pre_out.at[c], pre_in.at[c], pre_s.at[c], pre_r.at[c], z + 1, a)

    def suffix(c):
        return remote(suf_out.at[c], suf_in.at[c], suf_s.at[c], suf_r.at[c], z - 1, a)

    acc[...] = jnp.zeros_like(acc)
    mat[...] = jnp.zeros_like(mat)
    trial_load.wait()
    half[...] = trial[...].astype(bf16)
    gaps_load.wait()
    first = pl.multiple_of(a * share, 128)
    rows = share // 128

    def own_trial():
        return trial[:, pl.ds(first, share)]

    def own_gaps():
        return jnp.concatenate([gaps[pl.ds(a * rows + q, 1), :] for q in range(rows)], axis=1)

    eye = lax.broadcasted_iota(jnp.int32, (vecs, vecs), 0) == lax.broadcasted_iota(jnp.int32, (vecs, vecs), 1)

    def as_row(column):
        return jnp.sum(jnp.where(eye, column, 0.0), axis=0, keepdims=True)

    mine = own_trial()
    gram[...] = exact(mine, mine * own_gaps())
    pl.semaphore_wait(barrier, np_ - 1 + na - 1)

    after = np_ - 1 - z
    longest = jnp.maximum(z, after)

    def step(t, carry):
        @pl.when(t < chunks)
        def _():
            pltpu.make_async_copy(ints_hbm.at[:, pl.ds(0, width)], ints.at[t], load.at[t]).wait()
            own[t] = jnp.dot(half[...], ints[t], preferred_element_type=f32)

        p = t - LAG * z

        @pl.when((p >= 0) & (p < chunks) & (after > 0))
        def _():
            @pl.when(z == 0)
            def _():
                pre_out[p] = own[p].astype(bf16)

            @pl.when(z > 0)
            def _():
                prefix(p).wait_recv()
                pre_out[p] = (own[p] + pre_in[p].astype(f32)).astype(bf16)

            prefix(p).start()

        s = t - LAG * after

        @pl.when((s >= 0) & (s < chunks) & (z > 0))
        def _():
            @pl.when(after == 0)
            def _():
                suf_out[s] = own[s].astype(bf16)

            @pl.when(after > 0)
            def _():
                suffix(s).wait_recv()
                suf_out[s] = (own[s] + suf_in[s].astype(f32)).astype(bf16)

            suffix(s).start()

        c = t - LAG * longest

        @pl.when((c >= 0) & (c < chunks))
        def _():
            @pl.when(z == np_ - 1)
            def _():
                prefix(c).wait_recv()

            @pl.when(z == 0)
            def _():
                suffix(c).wait_recv()

            @pl.when(z > 0)
            def _():
                own[c] = own[c] + pre_in[c].astype(f32)

            @pl.when(after > 0)
            def _():
                own[c] = own[c] + suf_in[c].astype(f32)

            aux = own[c].astype(bf16)
            for b in range(chips):
                part = lax.dot_general(
                    aux, ints[c, pl.ds(b * 2 * share, 2 * share), :], NT, preferred_element_type=f32
                )
                acc[2 * b] += part[:, :share]
                acc[2 * b + 1] += part[:, share:]

            @pl.when(c % np_ == z)
            def _():
                total = own[c]
                mat[...] += exact(total, total.astype(bf16).astype(f32))

        return carry

    lax.fori_loop(0, chunks + LAG * (np_ - 1), step, 0)

    other = chip * 2 + 1 - core
    pending = []
    product = gram[...] + 2.0 * mat[...]
    mine = own_trial()
    squares = as_row(jnp.sum(mine * mine, axis=1, keepdims=True))
    h = vecs // 2
    m1_out[0:h] = jnp.concatenate([product[:h], product[h:]], axis=1)
    m1_out[h:] = jnp.broadcast_to(jnp.concatenate([squares, squares], axis=1), (8, 2 * vecs))
    m1_copy = remote(m1_out, m1_in, m1_s, m1_r, z, other)
    m1_copy.start()
    pending.append(m1_copy)

    b1 = []
    for d in range(chips):
        j = (chip + 1 + d) % chips
        b1_out[d] = acc[2 * j + 1 - core].astype(bf16)
        copy = remote(b1_out.at[d], b1_in.at[d], b1_s.at[d], b1_r.at[d], z, other)
        copy.start()
        b1.append(copy)
        pending.append(copy)
    m1_copy.wait_recv()
    m2[chip] = m1_out[...] + m1_in[...]
    for d in range(1, chips):
        copy = remote(m2.at[chip], m2.at[chip], m2_s.at[d], m2_r.at[chip], z, ((chip + d) % chips) * 2 + core)
        copy.start()
        pending.append(copy)
    for d in range(chips - 1):
        j = (chip + 1 + d) % chips
        b1[d].wait_recv()
        b2_out[d] = (acc[2 * j + core] + b1_in[d].astype(f32)).astype(bf16)
        copy = remote(b2_out.at[d], b2_in.at[d], b2_s.at[d], b2_r.at[d], z, 2 * j + core)
        copy.start()
        pending.append(copy)
    b1[chips - 1].wait_recv()
    coupled = acc[a] + b1_in[chips - 1].astype(f32)

    for d in range(1, chips):
        j = (chip + d) % chips
        remote(m2.at[j], m2.at[j], m2_s.at[d], m2_r.at[j], z, a).wait_recv()
    total = m2[0]
    for j in range(1, chips):
        total = total + m2[j]
    m3[z] = total
    for d in range(1, np_):
        copy = remote(m3.at[z], m3.at[z], m3_s.at[d], m3_r.at[z], (z + d) % np_, a)
        copy.start()
        pending.append(copy)

    for d in range(chips - 1):
        remote(b2_out.at[d], b2_in.at[d], b2_s.at[d], b2_r.at[d], z, a).wait_recv()
        coupled = coupled + b2_in[d].astype(f32)
    mine = own_trial()
    values = own_gaps() * mine + 2.0 * coupled
    sigma[...] = values
    lane = lax.broadcasted_iota(jnp.int32, (vecs, 128), 1)
    sums = jnp.where(
        lane == 0,
        jnp.sum(values * values, axis=1, keepdims=True),
        jnp.where(lane == 1, jnp.sum(values * mine, axis=1, keepdims=True), 0.0),
    )
    n1[a] = jnp.transpose(sums)[:8]
    for d in range(1, na):
        copy = remote(n1.at[a], n1.at[a], n1_s.at[d], n1_r.at[a], z, (a + d) % na)
        copy.start()
        pending.append(copy)
    outs = [pltpu.make_async_copy(sigma, sigma_hbm, store.at[0])]
    outs[0].start()
    for d in range(1, na):
        j = (a + d) % na
        remote(n1.at[j], n1.at[j], n1_s.at[d], n1_r.at[j], z, j).wait_recv()
    sums = n1[0]
    for j in range(1, na):
        sums = sums + n1[j]
    n2[z] = sums
    for d in range(1, np_):
        copy = remote(n2.at[z], n2.at[z], n2_s.at[d], n2_r.at[z], (z + d) % np_, a)
        copy.start()
        pending.append(copy)

    for d in range(1, np_):
        j = (z + d) % np_
        remote(m3.at[j], m3.at[j], m3_s.at[d], m3_r.at[j], j, a).wait_recv()
    total = m3[0]
    for j in range(1, np_):
        total = total + m3[j]
    pairs = float(np_ * na * share)
    subspace = jnp.concatenate([total[:h, :vecs], total[:h, vecs:]], axis=0) / pairs
    sub[...] = subspace
    outs.append(pltpu.make_async_copy(sub, sub_hbm, store.at[1]))
    outs[1].start()
    squares = total[h:h + 1, :vecs]
    diagonal = jnp.sum(jnp.where(eye, subspace, 0.0), axis=0, keepdims=True)
    rayleigh = diagonal / (squares / pairs + epsilon)
    column = jnp.sum(jnp.where(eye, rayleigh, 0.0), axis=1, keepdims=True)
    res[...] = sigma[...] - own_trial() * column
    outs.append(pltpu.make_async_copy(res, res_hbm, store.at[2]))
    outs[2].start()

    for d in range(1, np_):
        j = (z + d) % np_
        remote(n2.at[j], n2.at[j], n2_s.at[d], n2_r.at[j], j, a).wait_recv()
    sums = n2[0]
    for j in range(1, np_):
        sums = sums + n2[j]
    residual_sq = sums[0:1] - 2.0 * rayleigh * sums[1:2] + rayleigh * rayleigh * squares
    norm[...] = jnp.sqrt(residual_sq / pairs + epsilon)
    outs.append(pltpu.make_async_copy(norm, norm_hbm, store.at[3]))
    outs[3].start()

    @pl.when(after > 0)
    def _():
        for c in range(chunks):
            prefix(c).wait_send()

    @pl.when(z > 0)
    def _():
        for c in range(chunks):
            suffix(c).wait_send()

    for copy in pending:
        copy.wait_send()
    for copy in outs:
        copy.wait()


def store_kernel(*refs):
    for i in range(4):
        refs[i + 4][...] = refs[i][...]


def solution(mesh):
    np_, na = mesh.shape["pair"], mesh.shape["aux"]
    chips = na // 2

    def local(integrals, energy_gaps, trial_vectors):
        rows, cols = integrals.shape
        vecs = trial_vectors.shape[1]
        width = WIDTH
        chunks, share = cols // width, rows // na
        anywhere = pl.BlockSpec(memory_space=pl.ANY)
        dma = pltpu.SemaphoreType.DMA
        message = (vecs // 2 + 8, 2 * vecs)
        results = pl.pallas_call(
            functools.partial(kernel, np_, na, chunks, width, share),
            out_shape=[
                jax.ShapeDtypeStruct((vecs, share), f32),
                jax.ShapeDtypeStruct((vecs, vecs), f32),
                jax.ShapeDtypeStruct((vecs, share), f32),
                jax.ShapeDtypeStruct((1, vecs), f32),
            ],
            in_specs=[anywhere] * 3,
            out_specs=[anywhere] * 4,
            scratch_shapes=[
                pltpu.VMEM((chunks, rows, width), bf16),
                pltpu.VMEM((rows // 128, 128), f32),
                pltpu.VMEM((vecs, rows), f32),
                pltpu.VMEM((vecs, rows), bf16),
                pltpu.VMEM((chunks, vecs, width), f32),
                pltpu.VMEM((na, vecs, share), f32),
                pltpu.VMEM((vecs, vecs), f32),
                pltpu.VMEM((vecs, vecs), f32),
                *[pltpu.VMEM((chunks, vecs, width), bf16)] * 4,
                *[pltpu.VMEM((chips, vecs, share), bf16)] * 4,
                pltpu.VMEM(message, f32),
                pltpu.VMEM(message, f32),
                pltpu.VMEM((chips,) + message, f32),
                pltpu.VMEM((np_,) + message, f32),
                pltpu.VMEM((na, 8, vecs), f32),
                pltpu.VMEM((np_, 8, vecs), f32),
                pltpu.VMEM((vecs, share), f32),
                pltpu.VMEM((vecs, vecs), f32),
                pltpu.VMEM((vecs, share), f32),
                pltpu.VMEM((1, vecs), f32),
                dma((chunks,)), dma((2,)),
                dma((chunks,)), dma((chunks,)), dma((chunks,)), dma((chunks,)),
                dma((chips,)), dma((chips,)), dma((chips,)), dma((chips,)),
                dma, dma, dma((chips,)), dma((chips,)),
                dma((np_,)), dma((np_,)), dma((na,)), dma((na,)), dma((np_,)), dma((np_,)),
                dma((4,)),
            ],
            compiler_params=pltpu.CompilerParams(
                collective_id=0, has_side_effects=True, vmem_limit_bytes=VMEM
            ),
            name="sigma_build",
        )(integrals, energy_gaps.reshape(rows // 128, 128), trial_vectors.T)
        sigma, subspace, residuals, norms = pl.pallas_call(
            store_kernel,
            out_shape=[jax.ShapeDtypeStruct(x.shape, x.dtype) for x in results],
            in_specs=[pl.BlockSpec(memory_space=pltpu.VMEM)] * 4,
            out_specs=[pl.BlockSpec(memory_space=pltpu.VMEM)] * 4,
            compiler_params=pltpu.CompilerParams(vmem_limit_bytes=VMEM),
            name="store",
        )(*results)
        return sigma.T, subspace, residuals.T, norms.reshape(vecs)

    return jax.shard_map(
        local,
        mesh=mesh,
        in_specs=(P("pair", "aux"), P("pair"), P("pair", None)),
        out_specs=(P(("pair", "aux"), None), P(), P(("pair", "aux"), None), P()),
        check_vma=False,
    )
```
